8 devices in a mesh: data: 1 (over z), dap: 8 (over y, x, core).
Axes of the slice: x: 2, y: 2, z: 1, core: 2. Of those that a mesh axis runs over, the one named last changes fastest.
Arguments:
- z_one: bfloat16 [768, 768, 128], P(('data', 'dap'))
- mask_one: int32 [768, 768], P(('data', 'dap'))
- z_two: bfloat16 [768, 768, 128], P(('data', 'dap'))
- mask_two: int32 [768, 768], P(('data', 'dap'))
- norm_in: bfloat16 [2, 2, 128], replicated
- w_proj: bfloat16 [2, 128, 512], replicated
- w_gate: bfloat16 [2, 128, 128], replicated
- norm_mid: bfloat16 [2, 2, 128], replicated
- w_out: bfloat16 [2, 128, 128], replicated
Outputs:
- output 1: bfloat16 [768, 768, 128], P(('data', 'dap'))
- output 2: bfloat16 [768, 768, 128], P(('data', 'dap'))
All inputs are finite; a program needn't handle non-finite values.
Results may differ from the reference program's by a relative error of at most 0.00659121.
Values are sent between devices in bfloat16 or wider.
A program may use at most 1 GiB of HBM per device.

```python
import jax
import jax.numpy as jnp
from jax import lax

N = 768
CZ = 128
C = 128


def layer_norm(vals, ln_gain, ln_shift):
    vals = vals.astype(jnp.float32)
    row_mean = jnp.mean(vals, axis=-1, keepdims=True)
    centred = vals - row_mean
    row_var = jnp.mean(centred * centred, axis=-1, keepdims=True)
    return centred * lax.rsqrt(row_var + 1e-5) * ln_gain.astype(jnp.float32) + ln_shift.astype(jnp.float32)


def draw_mask(mask_key):
    residue_ok = (jax.random.randint(mask_key, (N,), 0, 20) != 0).astype(jnp.int32)
    return residue_ok[:, None] * residue_ok[None, :]


def setup_inputs(seed: int = 0, part: int = 0) -> dict:
    part_keys = jax.random.split(jax.random.fold_in(jax.random.key(seed), part), 4)
    shared_keys = jax.random.split(jax.random.key(seed + 1), 5)
    norm_base = jnp.array([1.0, 0.0], jnp.float32)[None, :, None]
    return {
        "z_one": jax.random.normal(part_keys[0], (N, N, CZ), jnp.float32).astype(jnp.bfloat16),
        "mask_one": draw_mask(part_keys[1]),
        "z_two": jax.random.normal(part_keys[2], (N, N, CZ), jnp.float32).astype(jnp.bfloat16),
        "mask_two": draw_mask(part_keys[3]),
        "norm_in": (0.3 * jax.random.normal(shared_keys[0], (2, 2, CZ), jnp.float32) + norm_base).astype(jnp.bfloat16),
        "w_proj": (jax.random.normal(shared_keys[1], (2, CZ, 4 * C), jnp.float32) * CZ ** -0.5).astype(jnp.bfloat16),
        "w_gate": (jax.random.normal(shared_keys[2], (2, CZ, CZ), jnp.float32) * CZ ** -0.5).astype(jnp.bfloat16),
        "norm_mid": (0.3 * jax.random.normal(shared_keys[3], (2, 2, C), jnp.float32) + norm_base).astype(jnp.bfloat16),
        "w_out": (jax.random.normal(shared_keys[4], (2, C, CZ), jnp.float32) * C ** -0.5).astype(jnp.bfloat16),
    }


def project_row(z_row, mask_row, norm_in, w_proj):
    x_row = layer_norm(z_row, norm_in[0], norm_in[1]).astype(jnp.bfloat16)
    projected = jnp.dot(x_row, w_proj, preferred_element_type=jnp.float32)
    keep_mask = mask_row.astype(jnp.float32)[:, None]
    a_row = keep_mask * jax.nn.sigmoid(projected[:, C:2 * C]) * projected[:, :C]
    b_row = keep_mask * jax.nn.sigmoid(projected[:, 3 * C:]) * projected[:, 2 * C:3 * C]
    return a_row.astype(jnp.bfloat16), b_row.astype(jnp.bfloat16)


def output_row(z_row, t_row, norm_in, w_gate, norm_mid, w_out):
    x_row = layer_norm(z_row, norm_in[0], norm_in[1]).astype(jnp.bfloat16)
    gate_val = jax.nn.sigmoid(jnp.dot(x_row, w_gate, preferred_element_type=jnp.float32))
    t_norm = layer_norm(t_row, norm_mid[0], norm_mid[1]).astype(jnp.bfloat16)
    update = jnp.dot(t_norm, w_out, preferred_element_type=jnp.float32)
    return (z_row.astype(jnp.float32) + gate_val * update).astype(jnp.bfloat16)


def tri_update(z_pair, pair_mask, norm_in, w_proj, w_gate, norm_mid, w_out, form):
    a_side, b_side = lax.map(lambda row_pair: project_row(row_pair[0], row_pair[1], norm_in, w_proj), (z_pair, pair_mask))
    tri_prod = jnp.einsum(form, a_side.astype(jnp.float32), b_side.astype(jnp.float32)).astype(jnp.bfloat16)
    return lax.map(lambda row_pair: output_row(row_pair[0], row_pair[1], norm_in, w_gate, norm_mid, w_out), (z_pair, tri_prod))


def run_crop(z_pair, pair_mask, norm_in, w_proj, w_gate, norm_mid, w_out):
    z_mid = tri_update(z_pair, pair_mask, norm_in[0], w_proj[0], w_gate[0], norm_mid[0], w_out[0], "ikc,jkc->ijc")
    return tri_update(z_mid, pair_mask, norm_in[1], w_proj[1], w_gate[1], norm_mid[1], w_out[1], "kic,kjc->ijc")


def reference(z_one, mask_one, z_two, mask_two, norm_in, w_proj, w_gate, norm_mid, w_out):
    return (run_crop(z_one, mask_one, norm_in, w_proj, w_gate, norm_mid, w_out),
            run_crop(z_two, mask_two, norm_in, w_proj, w_gate, norm_mid, w_out))
```

```python
import functools

import jax
import jax.numpy as jnp
from jax import lax
from jax.experimental import pallas as pl
from jax.experimental.pallas import tpu as pltpu
from jax.sharding import PartitionSpec as P

BF, F32 = jnp.bfloat16, jnp.float32
IB = 16
ST = 17
VMEM = 60 << 20


def norm_cols(vals, gain, shift):
    cen = vals - jnp.mean(vals, axis=0, keepdims=True)
    var = jnp.mean(cen * cen, axis=0, keepdims=True)
    return cen * lax.rsqrt(var + 1e-5) * gain + shift


def put_row(scr, i, side):
    for t in range(side.shape[1] // 128):
        scr[t, pl.ds(i, 128, stride=ST), :] = side[:, t * 128:(t + 1) * 128]


def drain(scr, out):
    for c in range(128):
        for t in range(out.shape[2] // 128):
            out[c, :, t * 128:(t + 1) * 128] = scr[t, c * ST:c * ST + IB, :].astype(BF)


def gated(q):
    return q[:128] * jnp.tanh(q[128:256]) + q[:128], q[256:384] * jnp.tanh(q[384:]) + q[256:384]


def dot(lhs, rhs):
    return jnp.dot(lhs, rhs, preferred_element_type=F32)


def params(*sem):
    return pltpu.CompilerParams(vmem_limit_bytes=VMEM, dimension_semantics=sem)


def proj_kernel(z_ref, m_ref, gain, shift, w_ref, *rest):
    a_ref, b_ref, sa, sb = rest[-4:]
    for i in range(IB):
        x = norm_cols(z_ref[i].T.astype(F32), gain[...], shift[...])
        a, b = gated(dot(w_ref[...], (x * m_ref[i:i + 1, :].astype(F32)).astype(BF)))
        put_row(sa, i, a)
        put_row(sb, i, b)
    drain(sa, a_ref)
    drain(sb, b_ref)


def proj(z, m, gain, shift, w, total, off, prev=()):
    rows, n, _ = z.shape
    kb = 256
    full = lambda shape: pl.BlockSpec(shape, lambda i, j: (0,) * len(shape))
    out = pl.BlockSpec((128, IB, kb), lambda i, j: (0, off // IB + i, j))
    return pl.pallas_call(
        proj_kernel, grid=(rows // IB, n // kb),
        in_specs=[pl.BlockSpec((IB, kb, 128), lambda i, j: (i, j, 0)),
                  pl.BlockSpec((IB, kb), lambda i, j: (i, j)),
                  full((128, kb)), full((128, kb)), full((512, 128))]
        + [pl.BlockSpec(memory_space=pl.ANY)] * len(prev),
        out_specs=[out, out],
        scratch_shapes=[pltpu.VMEM((kb // 128, 128 * ST, 128), F32)] * 2,
        out_shape=[jax.ShapeDtypeStruct((128, total, n), BF)] * 2,
        input_output_aliases={5 + k: k for k in range(len(prev))},
        compiler_params=params("arbitrary", "arbitrary"), name="proj")(z, m, gain, shift, w, *prev)


def tri_out_kernel(n_lhs, sc, *refs):
    lhs, rhs, out, buf = refs[:n_lhs], refs[n_lhs:n_lhs + 4], refs[n_lhs + 4], refs[n_lhs + 5]
    for g in range(out.shape[0]):
        for k, r in enumerate(rhs):
            buf[g, pl.ds(pl.multiple_of(sc[k] * 96, 16), 96), :] = r[g, 0]
        row = 0
        for l in lhs:
            m = l.shape[1]
            out[g, row:row + m, :] = lax.dot_general(
                l[g], buf[g], (((1,), (1,)), ((), ())), preferred_element_type=F32).astype(BF)
            row += m


def tri_out(sc, lhs, rhs):
    cb = 2
    n = lhs[0].shape[2]
    rows = sum(l.shape[1] for l in lhs)

    def rhs_spec(idx):
        return pl.BlockSpec((cb, 1, 96, n), lambda g, s: (g, 0 if idx is None else s[idx], 0, 0))

    return pl.pallas_call(
        functools.partial(tri_out_kernel, len(lhs)),
        grid_spec=pltpu.PrefetchScalarGridSpec(
            num_scalar_prefetch=1, grid=(128 // cb,),
            in_specs=[pl.BlockSpec((cb, l.shape[1], n), lambda g, s: (g, 0, 0)) for l in lhs]
            + [rhs_spec(i) for _, i in rhs],
            out_specs=pl.BlockSpec((cb, rows, 384), lambda g, s: (g, 0, 0)),
            scratch_shapes=[pltpu.VMEM((cb, 384, n), BF)]),
        out_shape=jax.ShapeDtypeStruct((128, rows, 384), BF),
        compiler_params=params("arbitrary"), name="tri_out")(
            sc, *lhs, *[r.reshape(128, r.shape[1] // 96, 96, n) for r, _ in rhs])


def stage_t(t_ref, st):
    for c in range(128):
        st[c * ST:c * ST + IB, :] = t_ref[c].astype(F32)


def pair_t(st, i):
    return jnp.concatenate([st[pl.ds(i, 128, stride=ST), :], st[pl.ds(i + 1, 128, stride=ST), :]], axis=1)


def mid_kernel(sc, t_ref, z_ref, m_ref, n_ref, wg, wo, w2, zm_ref, a_ref, b_ref, st, sa, sb):
    stage_t(t_ref, st)
    for i in range(0, IB, 2):
        zt = jnp.concatenate([z_ref[i].T, z_ref[i + 1].T], axis=1).astype(F32)
        gate = dot(wg[...], norm_cols(zt, n_ref[0], n_ref[1]).astype(BF))
        upd = dot(wo[...], norm_cols(pair_t(st, i), n_ref[2], n_ref[3]).astype(BF))
        zm = (zt + (upd * jnp.tanh(gate) + upd)).astype(BF)
        zm_ref[i], zm_ref[i + 1] = zm[:, :128], zm[:, 128:]
        keep = jnp.concatenate([m_ref[i:i + 1, :], m_ref[i + 1:i + 2, :]], axis=1).astype(F32)
        x2 = norm_cols(zm.astype(F32), n_ref[4], n_ref[5]) * keep
        a, b = gated(dot(w2[...], x2.astype(BF)))
        for r in range(2):
            put_row(sa, i + r, a[:, r * 128:(r + 1) * 128])
            put_row(sb, i + r, b[:, r * 128:(r + 1) * 128])
    drain(sa, a_ref)
    drain(sb, b_ref)


def mid(sc, half, t, t_row, z, m, norms, wg, wo, w2):
    rows = z.shape[0]
    full = lambda a: pl.BlockSpec(a.shape, lambda i, j, s: (0,) * a.ndim)
    side = pl.BlockSpec((128, IB, 128), lambda i, j, s: (0, i, j))
    return pl.pallas_call(
        mid_kernel,
        grid_spec=pltpu.PrefetchScalarGridSpec(
            num_scalar_prefetch=1, grid=(rows // IB, 3),
            in_specs=[pl.BlockSpec((128, IB, 128), lambda i, j, s: (0, t_row // IB + i, j)),
                      pl.BlockSpec((IB, 128, 128), lambda i, j, s: (i, 3 * s[half] + j, 0)),
                      pl.BlockSpec((IB, 128), lambda i, j, s: (i, 3 * s[half] + j)),
                      full(norms), full(wg), full(wo), full(w2)],
            out_specs=[pl.BlockSpec((IB, 128, 128), lambda i, j, s: (i, 0, j)), side, side],
            scratch_shapes=[pltpu.VMEM((128 * ST, 128), F32)] + [pltpu.VMEM((1, 128 * ST, 128), F32)] * 2),
        out_shape=[jax.ShapeDtypeStruct((rows, 128, 384), BF)] + [jax.ShapeDtypeStruct((128, rows, 384), BF)] * 2,
        compiler_params=params("arbitrary", "arbitrary"), name="mid")(sc, t, z, m, norms, wg, wo, w2)


def tri_in_kernel(ns, sel_a, off, sel_b, sc, *refs):
    out, abuf, bbuf = refs[-3:]
    ins = refs[:-3]

    def fill(buf, base, g):
        row = 0
        for r in ins[base * ns:(base + 2) * ns]:
            buf[row:row + r.shape[1], :] = r[g]
            row += r.shape[1]

    def product(g, lo):
        at = abuf[:, lo:lo + 256].T
        rows = at[lo // 2:lo // 2 + 192]
        out[g] = dot(rows, bbuf[...]).astype(BF)

    for g in range(out.shape[0]):
        if sel_a is None:
            fill(abuf, 0, g)
        else:
            pl.when(sc[sel_a] == 0)(lambda: fill(abuf, 0, g))
            pl.when(sc[sel_a] == 1)(lambda: fill(abuf, 2, g))
        nb = 2 if sel_a is None else 4
        pl.when(sc[sel_b] == 0)(lambda: fill(bbuf, nb, g))
        pl.when(sc[sel_b] == 1)(lambda: fill(bbuf, nb + 2, g))
        pl.when(sc[off] == 0)(lambda: product(g, 0))
        pl.when(sc[off] == 1)(lambda: product(g, 128))


def tri_in(sc, a_sets, b_sets, sel_a, off, sel_b):
    cb = 2
    ns = len(a_sets[0])

    def spec(arr, sel, want):
        shape = (cb,) + arr.shape[1:]
        if sel is None:
            return pl.BlockSpec(shape, lambda g, s: (g, 0, 0))
        return pl.BlockSpec(shape, lambda g, s: (jnp.where(s[sel] == want, g, 0), 0, 0))

    specs, args = [], []
    for k, group in enumerate(a_sets):
        specs += [spec(arr, sel_a, k // 2) for arr in group]
        args += list(group)
    for k, group in enumerate(b_sets):
        specs += [spec(arr, sel_b, k // 2) for arr in group]
        args += list(group)
    return pl.pallas_call(
        functools.partial(tri_in_kernel, ns, sel_a, off, sel_b),
        grid_spec=pltpu.PrefetchScalarGridSpec(
            num_scalar_prefetch=1, grid=(128 // cb,), in_specs=specs,
            out_specs=pl.BlockSpec((cb, 192, 384), lambda g, s: (g, 0, 0)),
            scratch_shapes=[pltpu.VMEM((768, 384), BF)] * 2),
        out_shape=jax.ShapeDtypeStruct((128, 192, 384), BF),
        compiler_params=params("arbitrary"), name="tri_in")(sc, *args)


def finish_kernel(sel, sc, t_ref, za_ref, zb_ref, n_ref, wg, wo, o_ref, st):
    stage_t(t_ref, st)
    half_a = sc[sel] == 0
    for i in range(0, IB, 2):
        zt = jnp.where(half_a, jnp.concatenate([za_ref[i], za_ref[i + 1]], axis=1),
                       jnp.concatenate([zb_ref[i], zb_ref[i + 1]], axis=1)).astype(F32)
        gate = dot(wg[...], norm_cols(zt, n_ref[4], n_ref[5]).astype(BF))
        upd = dot(wo[...], norm_cols(pair_t(st, i), n_ref[6], n_ref[7]).astype(BF))
        o = zt + (upd * jnp.tanh(gate) + upd)
        o_ref[i], o_ref[i + 1] = o[:, :128].T.astype(BF), o[:, 128:].T.astype(BF)


def finish(sc, row, sel, t, za, zb, norms, wg, wo):
    full = lambda a: pl.BlockSpec(a.shape, lambda i, j, s: (0,) * a.ndim)

    def zspec(want):
        def at(i, j, s):
            use = s[sel] == want
            return jnp.where(use, i, 0), 0, jnp.where(use, j, 0)
        return pl.BlockSpec((IB, 128, 128), at)

    return pl.pallas_call(
        functools.partial(finish_kernel, sel),
        grid_spec=pltpu.PrefetchScalarGridSpec(
            num_scalar_prefetch=1, grid=(96 // IB, 3),
            in_specs=[pl.BlockSpec((128, IB, 128), lambda i, j, s: (0, s[row] * (96 // IB) + i, j)),
                      zspec(0), zspec(1), full(norms), full(wg), full(wo)],
            out_specs=pl.BlockSpec((IB, 128, 128), lambda i, j, s: (i, j, 0)),
            scratch_shapes=[pltpu.VMEM((128 * ST, 128), F32)]),
        out_shape=jax.ShapeDtypeStruct((96, 384, 128), BF),
        compiler_params=params("arbitrary", "arbitrary"), name="finish")(sc, t, za, zb, norms, wg, wo)


def solution(mesh):
    row_spec = P(("data", "dap"), None, None)
    mask_spec = P(("data", "dap"), None)
    rep = P()

    chip_core = [(d // 2, d % 2) for d in range(8)]
    near = lambda chip, core: chip ^ (1 if core == 0 else 2)
    far = lambda chip, core: chip ^ (2 if core == 0 else 1)
    perm_x = [(near(p, c) * 2 + c, p * 2 + c) for p, c in chip_core]
    perm_w = [(far(p, c) * 2 + c, p * 2 + c) for p, c in chip_core]
    perm_d = [((p ^ 3) * 2 + c, p * 2 + c) for p, c in chip_core]
    perm_core = [(p * 2 + c, p * 2 + 1 - c) for p, c in chip_core]
    perm_a = [(p * 2 + 1 - p // 2, p * 2 + p // 2) for p in range(4)]
    perm_b = [(p * 2 + p // 2, p * 2 + 1 - p // 2) for p in range(4)]
    perm_cross = [(p * 2 + c, near(p, c) * 2 + 1 - c) for p, c in chip_core]
    perm_same = [(p * 2 + c, near(p, c) * 2 + c) for p, c in chip_core]
    send = lambda arr, perm: lax.ppermute(arr, "dap", perm)

    def per_device(z_one, mask_one, z_two, mask_two, norm_in, w_proj, w_gate, norm_mid, w_out):
        d = lax.axis_index("dap")
        core, chip = d % 2, d // 2
        x, y = chip % 2, chip // 2
        crop = (x + y) % 2
        i32 = lambda *v: jnp.stack([jnp.asarray(k, jnp.int32) for k in v])

        wide = lambda v, n: jnp.broadcast_to(v.astype(F32)[:, None], (128, n))
        norms = jnp.stack([wide(v, 256) for u in range(2) for v in
                           (norm_in[u, 0], norm_in[u, 1], norm_mid[u, 0], norm_mid[u, 1])])
        wp = [(w_proj[u].T * jnp.asarray(0.5, BF)) for u in range(2)]
        wg = [(w_gate[u].T * jnp.asarray(0.5, BF)) for u in range(2)]
        wo = [(w_out[u].T * jnp.asarray(0.5, BF)) for u in range(2)]

        first = crop == 0
        z_own, z_oth = jnp.where(first, z_one, z_two), jnp.where(first, z_two, z_one)
        m_own, m_oth = jnp.where(first, mask_one, mask_two), jnp.where(first, mask_two, mask_one)
        z_x, m_x = send(z_oth, perm_x), send(m_oth, perm_x)
        z_w, m_w = send(z_oth, perm_w), send(m_oth, perm_w)
        z_own_late, m_own_late, z_x, z_w = lax.optimization_barrier((z_own, m_own, z_x, z_w))
        z_d, m_d = send(z_own_late, perm_d), send(m_own_late, perm_d)

        pr = lambda z, m, total, off, prev=(): proj(z, m, norms[0], norms[1], wp[0], total, off, prev)
        a_o, b_o = pr(z_own, m_own, 96, 0)
        bo_o = send(b_o, perm_core)
        ab = pr(z_x, m_x, 192, 0)
        a_xw, b_xw = pr(z_w, m_w, 192, 96, ab)
        bo_xw = send(b_xw, perm_core)

        base = [x * 2 + core, x * 2 + 1 - core, (1 - x) * 2 + core, (1 - x) * 2 + 1 - core]
        sc_a = i32(*base, core, 1 - core)
        sc_b = i32(*base, 1 - core, core)
        t_a = tri_out(sc_a, [a_o, a_xw], [(b_o, None), (bo_o, None), (b_xw, 4), (bo_xw, 5)])

        sc_h = i32(y, 1 - y)
        md = lambda half, t, row, z, m: mid(sc_h, half, t, row, z, m, norms, wg[0], wo[0], wp[1])
        zs, am, bm = {}, {}, {}
        zs["oa"], am["oa"], bm["oa"] = md(0, t_a, 0, z_own, m_own)
        zs["xa"], am["xa"], bm["xa"] = md(0, t_a, 96, z_x, m_x)
        zs["wa"], am["wa"], bm["wa"] = md(0, t_a, 192, z_w, m_w)

        a_d, b_d = pr(z_d, m_d, 96, 0)
        bo_d = send(b_d, perm_core)
        t_b = tri_out(sc_b, [a_o, a_xw, a_d], [(b_xw, 4), (bo_xw, 5), (b_d, None), (bo_d, None)])
        t_da = tri_out(sc_a, [a_d], [(b_o, None), (bo_o, None), (b_xw, 4), (bo_xw, 5)])
        zs["ob"], am["ob"], bm["ob"] = md(1, t_b, 0, z_own, m_own)
        zs["xb"], am["xb"], bm["xb"] = md(1, t_b, 96, z_x, m_x)
        zs["wb"], am["wb"], bm["wb"] = md(1, t_b, 192, z_w, m_w)
        _, am["db"], bm["db"] = md(1, t_b, 288, z_d, m_d)
        _, am["da"], bm["da"] = md(0, t_da, 0, z_d, m_d)

        ao = {k: send(v, perm_core) for k, v in am.items()}
        bo = {k: send(v, perm_a if k[1] == "a" else perm_b) for k, v in bm.items()}
        zo = {k: send(zs[k], perm_a if k[1] == "a" else perm_b) for k in ("oa", "wa", "ob", "wb")}

        group = lambda arrs, h: [arrs[s + h] for s in "oxwd"]
        b_sets = [group(bm, "a"), group(bo, "a"), group(bm, "b"), group(bo, "b")]
        a_all = [group(am, "a"), group(ao, "a"), group(am, "b"), group(ao, "b")]
        keep_b = jnp.where(core == y, 0, 1)
        sc_i = i32(core, jnp.where(core == 0, 1 - x, x), x, keep_b, core, 1 - core)
        fin = lambda row, t, za, zb: finish(sc_i, row, 3, t, za, zb, norms, wg[1], wo[1])
        t_near = tri_in(sc_i, a_all, b_sets, 0, 1, 3)
        r_same = send(fin(4, t_near, zs["xa"], zs["xb"]), perm_same)
        r_cross = send(fin(5, t_near, zo["wa"], zo["wb"]), perm_cross)
        t_own = tri_in(sc_i, a_all[:2], b_sets, None, 2, 3)
        r_core = send(fin(5, t_own, zo["oa"], zo["ob"]), perm_core)
        r_keep = fin(4, t_own, zs["oa"], zs["ob"])

        lo_core = core == 0
        outs = []
        for own in (first, jnp.logical_not(first)):
            mine, yours = jnp.where(own, r_keep, r_same), jnp.where(own, r_core, r_cross)
            outs.append(jnp.concatenate([jnp.where(lo_core, mine, yours), jnp.where(lo_core, yours, mine)], axis=1))
        return tuple(outs)

    return jax.shard_map(per_device, mesh=mesh,
                         in_specs=(row_spec, mask_spec, row_spec, mask_spec, rep, rep, rep, rep, rep),
                         out_specs=(row_spec, row_spec), check_vma=False)
```
